32 devices in a mesh: replica: 8 (over z, y), model: 4 (over x, core).
Axes of the slice: x: 2, y: 2, z: 4, core: 2. Of those that a mesh axis runs over, the one named last changes fastest.
Arguments:
- slope_up: float32 [8, 1024, 4096], P('replica', None, 'model'), may hold values from -4 to 4
- slope_down: float32 [8, 4096, 1024], P('replica', 'model'), may hold values from -4 to 4
- slope_query: float32 [8, 1024, 1024], P('replica', None, 'model'), may hold values from -4 to 4
- slope_key: float32 [8, 1024, 1024], P('replica', None, 'model'), may hold values from -4 to 4
- slope_value: float32 [8, 1024, 1024], P('replica', None, 'model'), may hold values from -4 to 4
- slope_mixed: float32 [8, 1024, 1024], P('replica', 'model'), may hold values from -4 to 4
- slope_norm: float32 [8, 1024], P('replica'), may hold values from -8 to 8
- slope_bias: float32 [8, 1024], P('replica'), may hold values from -8 to 8
- param_up: float32 [1024, 4096], P('replica', 'model'), may hold values from -0.25 to 0.25
- param_down: float32 [4096, 1024], P('model', 'replica'), may hold values from -0.125 to 0.125
- param_query: float32 [1024, 1024], P('replica', 'model'), may hold values from -0.25 to 0.25
- param_key: float32 [1024, 1024], P('replica', 'model'), may hold values from -0.25 to 0.25
- param_value: float32 [1024, 1024], P('replica', 'model'), may hold values from -0.25 to 0.25
- param_mixed: float32 [1024, 1024], P('model', 'replica'), may hold values from -0.25 to 0.25
- param_norm: float32 [1024], P('replica'), may hold values from 0.25 to 1.75
- param_bias: float32 [1024], P('replica'), may hold values from -3 to 3
- state_up: float32 [1024, 4096], P('replica', 'model'), may hold values from 0.0001953125 to 0.001953125
- state_down: float32 [4096, 1024], P('model', 'replica'), may hold values from 4.8828126e-05 to 0.00048828125
- state_query: float32 [1024, 1024], P('replica', 'model'), may hold values from 0.0001953125 to 0.001953125
- state_key: float32 [1024, 1024], P('replica', 'model'), may hold values from 0.0001953125 to 0.001953125
- state_value: float32 [1024, 1024], P('replica', 'model'), may hold values from 0.0001953125 to 0.001953125
- state_mixed: float32 [1024, 1024], P('model', 'replica'), may hold values from 0.0001953125 to 0.001953125
- state_norm: float32 [1024], P('replica'), may hold values from 0.05 to 0.8
- state_bias: float32 [1024], P('replica'), may hold values from 0.05 to 0.8
Outputs:
- half_up: bfloat16 [1024, 4096], P(None, 'model')
- half_down: bfloat16 [4096, 1024], P('model')
- half_query: bfloat16 [1024, 1024], P(None, 'model')
- half_key: bfloat16 [1024, 1024], P(None, 'model')
- half_value: bfloat16 [1024, 1024], P(None, 'model')
- half_mixed: bfloat16 [1024, 1024], P('model')
- half_norm: bfloat16 [1024], replicated
- half_bias: bfloat16 [1024], replicated
- next_up: float32 [1024, 4096], P('replica', 'model')
- next_down: float32 [4096, 1024], P('model', 'replica')
- next_query: float32 [1024, 1024], P('replica', 'model')
- next_key: float32 [1024, 1024], P('replica', 'model')
- next_value: float32 [1024, 1024], P('replica', 'model')
- next_mixed: float32 [1024, 1024], P('model', 'replica')
- next_norm: float32 [1024], P('replica')
- next_bias: float32 [1024], P('replica')
- state_new_up: float32 [1024, 4096], P('replica', 'model')
- state_new_down: float32 [4096, 1024], P('model', 'replica')
- state_new_query: float32 [1024, 1024], P('replica', 'model')
- state_new_key: float32 [1024, 1024], P('replica', 'model')
- state_new_value: float32 [1024, 1024], P('replica', 'model')
- state_new_mixed: float32 [1024, 1024], P('model', 'replica')
- state_new_norm: float32 [1024], P('replica')
- state_new_bias: float32 [1024], P('replica')
The draws below stay inside these ranges and needn't reach their ends.
All inputs are finite; a program needn't handle non-finite values.
Results may differ from the reference program's by a relative error of at most 0.001.
Values may be sent and summed in bfloat16 or wider, within the bound.
A program may use at most 64 MiB of HBM per device.

```python
import jax
import jax.numpy as jnp
from jax import lax

WIDTH = 1024
INNER = 4096
ATTN = 1024
REPLICAS = 8


def strengthened(drawn, own_key, source, target, parts, factor):
    owner, partner = [(jnp.arange(drawn.shape[axis_at]) // (drawn.shape[axis_at] // parts)).reshape([-1 if axis == axis_at else 1 for axis in range(drawn.ndim)]) for axis_at in (source, target)]
    chosen = jax.random.permutation(own_key, parts)[partner]
    strong = (owner == chosen) | (owner == (partner + parts // 2) % parts)
    return jnp.where(strong, factor * drawn, drawn)


def shard_levels(rng, dims, split, least, top_value):
    level, own = 1.0, jax.random.fold_in(rng, 6)
    for axis_at, blocks in split:
        heights = jnp.exp(jax.random.uniform(jax.random.fold_in(own, axis_at), (blocks,), jnp.float32, least / len(split), top_value / len(split)))
        level = level * jnp.repeat(heights, dims[axis_at] // blocks).reshape([-1 if axis == axis_at else 1 for axis in range(len(dims))])
    return level


def noise(own_key, shape, scale, reach, shards=(), kind=jnp.bfloat16):
    loudness = shard_levels(own_key, shape, shards, -0.22, 0.18) if shards else 1.0
    drawn = jax.random.normal(own_key, shape, jnp.float32) * scale * loudness
    return jnp.minimum(jnp.maximum(drawn, -reach), reach).astype(kind)


def heavy_noise(stream_key, dims, deviation, most, cuts, heavy, kind=jnp.bfloat16):
    array = deviation * jax.random.normal(stream_key, dims, jnp.float32)
    if cuts:
        array = array * shard_levels(stream_key, dims, cuts, -0.22, 0.18)
    return jnp.clip(strengthened(array, jax.random.fold_in(stream_key, 3), *heavy), -most, most).astype(kind)


def setup_inputs(seed: int = 0) -> dict:
    key_of = jax.random.split(jax.random.key(seed), 25)
    return {
        "slope_up": heavy_noise(key_of[0], (REPLICAS, WIDTH, INNER), 0.5, 4.0, ((0, 8), (2, 4)), (0, 1, 8, 2.0), jnp.float32),
        "slope_down": heavy_noise(key_of[1], (REPLICAS, INNER, WIDTH), 0.5, 4.0, ((0, 8), (1, 4)), (0, 2, 8, 2.0), jnp.float32),
        "slope_query": heavy_noise(key_of[2], (REPLICAS, WIDTH, ATTN), 0.5, 4.0, ((0, 8), (2, 4)), (0, 1, 8, 2.0), jnp.float32),
        "slope_key": heavy_noise(key_of[3], (REPLICAS, WIDTH, ATTN), 0.5, 4.0, ((0, 8), (2, 4)), (0, 1, 8, 2.0), jnp.float32),
        "slope_value": heavy_noise(key_of[4], (REPLICAS, WIDTH, ATTN), 0.5, 4.0, ((0, 8), (2, 4)), (0, 1, 8, 2.0), jnp.float32),
        "slope_mixed": heavy_noise(key_of[5], (REPLICAS, ATTN, WIDTH), 0.5, 4.0, ((0, 8), (1, 4)), (0, 2, 8, 2.0), jnp.float32),
        "slope_norm": heavy_noise(key_of[6], (REPLICAS, WIDTH), 1.0, 8.0, ((0, 8),), (0, 1, 8, 2.0), jnp.float32),
        "slope_bias": heavy_noise(key_of[7], (REPLICAS, WIDTH), 1.0, 8.0, ((0, 8),), (0, 1, 8, 2.0), jnp.float32),
        "param_up": heavy_noise(key_of[8], (WIDTH, INNER), WIDTH ** -0.5, 0.25, ((0, 8), (1, 4)), (1, 0, 8, 2.0), jnp.float32),
        "param_down": heavy_noise(key_of[9], (INNER, WIDTH), INNER ** -0.5, 0.125, ((0, 4), (1, 8)), (0, 1, 8, 2.0), jnp.float32),
        "param_query": heavy_noise(key_of[10], (WIDTH, ATTN), WIDTH ** -0.5, 0.25, ((0, 8), (1, 4)), (1, 0, 8, 2.0), jnp.float32),
        "param_key": heavy_noise(key_of[11], (WIDTH, ATTN), WIDTH ** -0.5, 0.25, ((0, 8), (1, 4)), (1, 0, 8, 2.0), jnp.float32),
        "param_value": heavy_noise(key_of[12], (WIDTH, ATTN), WIDTH ** -0.5, 0.25, ((0, 8), (1, 4)), (1, 0, 8, 2.0), jnp.float32),
        "param_mixed": heavy_noise(key_of[13], (ATTN, WIDTH), ATTN ** -0.5, 0.25, ((0, 4), (1, 8)), (0, 1, 8, 2.0), jnp.float32),
        "param_norm": jnp.clip(1.0 + 0.15 * jax.random.normal(key_of[14], (WIDTH,), jnp.float32), 0.25, 1.75),
        "param_bias": noise(key_of[15], (WIDTH,), 0.5, 3.0, ((0, 8),), jnp.float32),
        "state_up": jnp.clip(0.0001953125 + 0.0017578125 * jax.random.uniform(key_of[16], (WIDTH, INNER), jnp.float32) ** shard_levels(key_of[16], (WIDTH, INNER), ((0, 8), (1, 4)), -0.2, 0.2), 0.0001953125, 0.001953125),
        "state_down": jnp.clip(4.882812572759576e-05 + 0.0004394531 * jax.random.uniform(key_of[17], (INNER, WIDTH), jnp.float32) ** shard_levels(key_of[17], (INNER, WIDTH), ((0, 4), (1, 8)), -0.2, 0.2), 4.882812572759576e-05, 0.00048828125),
        "state_query": jnp.clip(0.0001953125 + 0.0017578125 * jax.random.uniform(key_of[18], (WIDTH, ATTN), jnp.float32) ** shard_levels(key_of[18], (WIDTH, ATTN), ((0, 8), (1, 4)), -0.2, 0.2), 0.0001953125, 0.001953125),
        "state_key": jnp.clip(0.0001953125 + 0.0017578125 * jax.random.uniform(key_of[19], (WIDTH, ATTN), jnp.float32) ** shard_levels(key_of[19], (WIDTH, ATTN), ((0, 8), (1, 4)), -0.2, 0.2), 0.0001953125, 0.001953125),
        "state_value": jnp.clip(0.0001953125 + 0.0017578125 * jax.random.uniform(key_of[20], (WIDTH, ATTN), jnp.float32) ** shard_levels(key_of[20], (WIDTH, ATTN), ((0, 8), (1, 4)), -0.2, 0.2), 0.0001953125, 0.001953125),
        "state_mixed": jnp.clip(0.0001953125 + 0.0017578125 * jax.random.uniform(key_of[21], (ATTN, WIDTH), jnp.float32) ** shard_levels(key_of[21], (ATTN, WIDTH), ((0, 4), (1, 8)), -0.2, 0.2), 0.0001953125, 0.001953125),
        "state_norm": jnp.clip(0.05 + 0.75 * jax.random.uniform(key_of[22], (WIDTH,), jnp.float32) ** shard_levels(key_of[22], (WIDTH,), ((0, 8),), -0.2, 0.2), 0.05, 0.8),
        "state_bias": jnp.clip(0.05 + 0.75 * jax.random.uniform(key_of[23], (WIDTH,), jnp.float32) ** shard_levels(key_of[23], (WIDTH,), ((0, 8),), -0.2, 0.2), 0.05, 0.8),
    }


learn_rate = 0.025
hold_rate = 0.7

def reference(slope_up, slope_down, slope_query, slope_key, slope_value, slope_mixed, slope_norm, slope_bias, param_up, param_down, param_query, param_key, param_value, param_mixed, param_norm, param_bias, state_up, state_down, state_query, state_key, state_value, state_mixed, state_norm, state_bias):
    mean_up = lax.optimization_barrier(jnp.sum(slope_up.astype(jnp.float32), axis=0)) * REPLICAS ** (-0.5)
    mean_down = lax.optimization_barrier(jnp.sum(slope_down.astype(jnp.float32), axis=0)) * REPLICAS ** (-0.5)
    mean_query = lax.optimization_barrier(jnp.sum(slope_query.astype(jnp.float32), axis=0)) * REPLICAS ** (-0.5)
    mean_key = lax.optimization_barrier(jnp.sum(slope_key.astype(jnp.float32), axis=0)) * REPLICAS ** (-0.5)
    mean_value = lax.optimization_barrier(jnp.sum(slope_value.astype(jnp.float32), axis=0)) * REPLICAS ** (-0.5)
    mean_mixed = lax.optimization_barrier(jnp.sum(slope_mixed.astype(jnp.float32), axis=0)) * REPLICAS ** (-0.5)
    mean_norm = lax.optimization_barrier(jnp.sum(slope_norm.astype(jnp.float32), axis=0)) * REPLICAS ** (-0.5)
    mean_bias = lax.optimization_barrier(jnp.sum(slope_bias.astype(jnp.float32), axis=0)) * REPLICAS ** (-0.5)
    ratio_up = jnp.sqrt(lax.optimization_barrier(jnp.sum(param_up * param_up, axis=1, keepdims=True))) * lax.rsqrt(lax.optimization_barrier(jnp.sum(mean_up * mean_up, axis=1, keepdims=True)) + 1e-06)
    mean_up = mean_up * ratio_up
    ratio_down = jnp.sqrt(lax.optimization_barrier(jnp.sum(param_down * param_down, axis=0, keepdims=True))) * lax.rsqrt(lax.optimization_barrier(jnp.sum(mean_down * mean_down, axis=0, keepdims=True)) + 1e-06)
    mean_down = mean_down * ratio_down
    ratio_query = jnp.sqrt(lax.optimization_barrier(jnp.sum(param_query * param_query, axis=1, keepdims=True))) * lax.rsqrt(lax.optimization_barrier(jnp.sum(mean_query * mean_query, axis=1, keepdims=True)) + 1e-06)
    mean_query = mean_query * ratio_query
    ratio_key = jnp.sqrt(lax.optimization_barrier(jnp.sum(param_key * param_key, axis=1, keepdims=True))) * lax.rsqrt(lax.optimization_barrier(jnp.sum(mean_key * mean_key, axis=1, keepdims=True)) + 1e-06)
    mean_key = mean_key * ratio_key
    ratio_value = jnp.sqrt(lax.optimization_barrier(jnp.sum(param_value * param_value, axis=1, keepdims=True))) * lax.rsqrt(lax.optimization_barrier(jnp.sum(mean_value * mean_value, axis=1, keepdims=True)) + 1e-06)
    mean_value = mean_value * ratio_value
    ratio_mixed = jnp.sqrt(lax.optimization_barrier(jnp.sum(param_mixed * param_mixed, axis=0, keepdims=True))) * lax.rsqrt(lax.optimization_barrier(jnp.sum(mean_mixed * mean_mixed, axis=0, keepdims=True)) + 1e-06)
    mean_mixed = mean_mixed * ratio_mixed
    state_new_up = hold_rate * state_up + (1.0 - hold_rate) * mean_up * mean_up
    next_up = param_up - learn_rate * mean_up * lax.rsqrt(state_new_up + 1e-06)
    state_new_down = hold_rate * state_down + (1.0 - hold_rate) * mean_down * mean_down
    next_down = param_down - learn_rate * mean_down * lax.rsqrt(state_new_down + 1e-06)
    state_new_query = hold_rate * state_query + (1.0 - hold_rate) * mean_query * mean_query
    next_query = param_query - learn_rate * mean_query * lax.rsqrt(state_new_query + 1e-06)
    state_new_key = hold_rate * state_key + (1.0 - hold_rate) * mean_key * mean_key
    next_key = param_key - learn_rate * mean_key * lax.rsqrt(state_new_key + 1e-06)
    state_new_value = hold_rate * state_value + (1.0 - hold_rate) * mean_value * mean_value
    next_value = param_value - learn_rate * mean_value * lax.rsqrt(state_new_value + 1e-06)
    state_new_mixed = hold_rate * state_mixed + (1.0 - hold_rate) * mean_mixed * mean_mixed
    next_mixed = param_mixed - learn_rate * mean_mixed * lax.rsqrt(state_new_mixed + 1e-06)
    state_new_norm = hold_rate * state_norm + (1.0 - hold_rate) * mean_norm * mean_norm
    next_norm = param_norm - learn_rate * mean_norm * lax.rsqrt(state_new_norm + 1e-06)
    state_new_bias = hold_rate * state_bias + (1.0 - hold_rate) * mean_bias * mean_bias
    next_bias = param_bias - learn_rate * mean_bias * lax.rsqrt(state_new_bias + 1e-06)
    half_up = next_up.astype(jnp.bfloat16)
    half_down = next_down.astype(jnp.bfloat16)
    half_query = next_query.astype(jnp.bfloat16)
    half_key = next_key.astype(jnp.bfloat16)
    half_value = next_value.astype(jnp.bfloat16)
    half_mixed = next_mixed.astype(jnp.bfloat16)
    half_norm = next_norm.astype(jnp.bfloat16)
    half_bias = next_bias.astype(jnp.bfloat16)
    return (half_up, half_down, half_query, half_key, half_value, half_mixed, half_norm, half_bias, next_up, next_down, next_query, next_key, next_value, next_mixed, next_norm, next_bias, state_new_up, state_new_down, state_new_query, state_new_key, state_new_value, state_new_mixed, state_new_norm, state_new_bias)
```

```python
import functools

import jax
import jax.numpy as jnp
from jax import lax
from jax.experimental import pallas as pl
from jax.experimental.pallas import tpu as pltpu
from jax.sharding import PartitionSpec as P

learn_rate = 0.025
hold_rate = 0.7
root = 9
MESH = pl.DeviceIdType.MESH


class Group:
    def __init__(self, members, rows, near_first):
        self.members = members
        self.rows = rows
        self.near_first = near_first


UP, DOWN, MIXED, QKV = range(4)
GROUPS = (
    Group((0,), True, False),
    Group((1,), False, False),
    Group((5,), False, False),
    Group((2, 3, 4), True, True),
)
ORDER = ((1, 1), (0, 1), (1, 0), (0, 0))


def kernel(replicas, models, limit, shapes, *refs):
    slopes, slope_norm, slope_bias = refs[0:6], refs[6], refs[7]
    params, param_norm, param_bias = refs[8:14], refs[14], refs[15]
    states, state_norm, state_bias = refs[16:22], refs[22], refs[23]
    halves, half_norm, half_bias = refs[24:30], refs[30], refs[31]
    nexts, next_norm, next_bias = refs[32:38], refs[38], refs[39]
    news, new_norm, new_bias = refs[40:46], refs[46], refs[47]
    scratch = list(refs[48:])
    groups = range(len(GROUPS))
    take = lambda: [scratch.pop(0) for _ in groups]
    xin, enc1, rec1, enc2, rec2, enc3, rec3, own, st, full, sq, sqr = (take() for _ in range(12))
    vs, vown, vrec, vnext, vag = (scratch.pop(0) for _ in range(5))
    rs_s, rs_r, ag_s, ag_r, n_s, n_r, v_s, v_r, w_s, w_r = (scratch.pop(0) for _ in range(10))
    load_sem, own_sem, st_sem, half_sem, next_sem, new_sem, vown_sem = scratch

    r = lax.axis_index("replica")
    m = lax.axis_index("model")
    far, near, y = r // 4, (r // 2) % 2, r % 2
    bit = lambda v, k: v if k == 0 else 1 - v
    place = lambda k2, k1, ky: (bit(far, k2) * 2 + bit(near, k1)) * 2 + bit(y, ky)
    y_peer, near_peer, far_peer = place(0, 0, 1), place(0, 1, 0), place(1, 0, 0)

    scale = 2.0**13 / (limit * replicas)
    rate = replicas ** (-0.5)

    def encode(x):
        t = x * scale
        t2 = t * t
        t4 = t2 * t2
        return (t4 * t4 * t).astype(jnp.bfloat16)

    def decode(c):
        f = c.astype(jnp.float32)
        a = jnp.exp(jnp.log(jnp.abs(f)) * (1.0 / root)) * (1.0 / scale)
        return jnp.where(f < 0, -a, a)

    def block(g, kf, ks, kt):
        return kt * 4 + (kf * 2 + ks if GROUPS[g].near_first else ks * 2 + kf)

    def slab(g, b, ref, i):
        at = place(b // 4, (b // 2) % 2, b % 2)
        h, w = shapes[g]
        if GROUPS[g].rows:
            return ref.at[pl.ds(pl.multiple_of(at * h, h), h), :]
        return ref.at[:, pl.ds(pl.multiple_of(at * w, w), w)]

    def lanes(g, ref, i):
        n = len(GROUPS[g].members)
        w = shapes[g][1] // n
        return ref if n == 1 else ref.at[:, i * w : (i + 1) * w]

    def loop(g, body):
        h, w = shapes[g]
        step = min(h, max(16, 16 * 1024 // w // 16 * 16))
        while h % step:
            step -= 16
        lax.fori_loop(0, h // step, lambda i, c: (body(pl.ds(pl.multiple_of(i * step, step), step)), c)[1], 0)

    def remote(src, dst, s, d, peer, axis="replica"):
        return pltpu.make_async_remote_copy(
            src_ref=src, dst_ref=dst, send_sem=s, recv_sem=d, device_id={axis: peer}, device_id_type=MESH
        )

    barrier = pltpu.get_barrier_semaphore()
    for j in range(1, replicas):
        pl.semaphore_signal(barrier, inc=1, device_id={"replica": lax.rem(r + j, replicas)}, device_id_type=MESH)
    for j in range(1, models):
        pl.semaphore_signal(barrier, inc=1, device_id={"model": lax.rem(m + j, models)}, device_id_type=MESH)

    def load(g, b):
        for i, a in enumerate(GROUPS[g].members):
            pltpu.make_async_copy(
                slab(g, b, slopes[a].at[0], i), lanes(g, xin[g].at[b], i), load_sem.at[g, b]
            ).start()

    def loaded(g, b):
        pltpu.make_async_copy(xin[g].at[b], xin[g].at[b], load_sem.at[g, b]).wait()

    for kt, ks in ORDER:
        load(UP, block(UP, 1, ks, kt))
        load(QKV, block(QKV, 1, ks, kt))
    for kt, ks in ORDER:
        load(QKV, block(QKV, 0, ks, kt))
    for g in (DOWN, MIXED):
        for kt, ks in ORDER:
            load(g, block(g, 1, ks, kt))
    for g in groups:
        for i, a in enumerate(GROUPS[g].members):
            pltpu.make_async_copy(params[a], lanes(g, own[g], i), own_sem.at[g]).start()
            pltpu.make_async_copy(states[a], lanes(g, st[g], i), st_sem.at[g]).start()
    for g in (UP, DOWN, MIXED):
        for kt, ks in ORDER:
            load(g, block(g, 0, ks, kt))

    def peer_of(g, stage):
        if stage == 3:
            return far_peer
        return near_peer if (stage == 1) == GROUPS[g].near_first else y_peer

    def copy1(g, i):
        return remote(enc1[g].at[i], rec1[g].at[i], rs_s.at[g, i], rs_r.at[g, i], peer_of(g, 1))

    def copy2(g, kt):
        return remote(enc2[g].at[kt], rec2[g].at[kt], rs_s.at[g, 4 + kt], rs_r.at[g, 4 + kt], peer_of(g, 2))

    def copy3(g):
        return remote(enc3[g], rec3[g], rs_s.at[g, 6], rs_r.at[g, 6], peer_of(g, 3))

    def encode1(g, i):
        kt, ks = ORDER[i]
        b = block(g, 1, ks, kt)
        loaded(g, b)
        src, dst = xin[g].at[b], enc1[g].at[i]

        def body(d):
            dst[d, :] = encode(src[d, :])

        loop(g, body)

    def add(g, b, rec):
        acc = xin[g].at[b]

        def body(d):
            acc[d, :] = acc[d, :] + decode(rec[d, :])

        loop(g, body)

    def add_encode(g, b, rec, dst):
        acc = xin[g].at[b]

        def body(d):
            dst[d, :] = encode(acc[d, :] + decode(rec[d, :]))

        loop(g, body)

    def take1(g, i):
        kt, ks = ORDER[i]
        b = block(g, 0, ks, kt)
        loaded(g, b)
        copy1(g, i).wait_recv()
        if ks:
            add_encode(g, b, rec1[g].at[i], enc2[g].at[kt])
            copy2(g, kt).start()
        else:
            add(g, b, rec1[g].at[i])

    def take2(g, kt):
        b = block(g, 0, 0, kt)
        copy2(g, kt).wait_recv()
        if kt:
            add_encode(g, b, rec2[g].at[kt], enc3[g])
            copy3(g).start()
        else:
            add(g, b, rec2[g].at[kt])

    def fold(x):
        w = x.shape[1]
        total = x[:, 0:128]
        for k in range(128, w, 128):
            total = total + x[:, k : k + 128]
        return total

    def squares(g, which, read):
        h, w = shapes[g]
        if GROUPS[g].rows:
            n = len(GROUPS[g].members)

            def body(d):
                v = read(d)
                v = v * v
                for i in range(n):
                    sq[g][which, i, d, :] = fold(v[:, i * (w // n) : (i + 1) * (w // n)])

            loop(g, body)
        else:
            sq[g][which] = jnp.zeros((8, w), jnp.float32)

            def body(d):
                v = read(d)
                sq[g][which] += jnp.sum((v * v).reshape(-1, 8, w), axis=0)

            loop(g, body)

    def copyn(g, j):
        return remote(
            sq[g], sqr[g].at[j - 1], n_s.at[g, j - 1], n_r.at[g, j - 1], lax.rem(m + j, models), "model"
        )

    def own_squares(g):
        pltpu.make_async_copy(own[g], own[g], own_sem.at[g]).wait()
        squares(g, 0, lambda d: own[g][d, :])

    def take3(g):
        copy3(g).wait_recv()
        acc, rec = xin[g].at[0], rec3[g]

        def read(d):
            v = (acc[d, :] + decode(rec[d, :])) * rate
            acc[d, :] = v
            return v

        squares(g, 1, read)
        for j in range(1, models):
            copyn(g, j).start()

    def rule(p, s, v):
        s = hold_rate * s + (1.0 - hold_rate) * v * v
        return p - learn_rate * v * lax.rsqrt(s + 1e-06), s

    def update(g):
        h, w = shapes[g]
        for j in range(1, models):
            copyn(g, j).wait_recv()
        pltpu.make_async_copy(st[g], st[g], st_sem.at[g]).wait()
        acc, half = xin[g].at[0], full[g].at[0]

        def ratio(index, axis):
            p, s = sq[g][(0, *index)], sq[g][(1, *index)]
            for j in range(models - 1):
                p = p + sqr[g][(j, 0, *index)]
                s = s + sqr[g][(j, 1, *index)]
            p = jnp.sum(p, axis=axis, keepdims=True)
            s = jnp.sum(s, axis=axis, keepdims=True)
            return jnp.sqrt(p) * lax.rsqrt(s + 1e-06)

        if GROUPS[g].rows:
            n = len(GROUPS[g].members)

            def body(d):
                for i in range(n):
                    cols = slice(i * (w // n), (i + 1) * (w // n))
                    v = acc[d, cols] * ratio((i, d), 1)
                    p, s = rule(own[g][d, cols], st[g][d, cols], v)
                    own[g][d, cols] = p
                    st[g][d, cols] = s
                    half[d, cols] = p.astype(jnp.bfloat16)

            loop(g, body)
        else:
            t = ratio((), 0)

            def body(d):
                p, s = rule(own[g][d, :], st[g][d, :], acc[d, :] * t)
                own[g][d, :] = p
                st[g][d, :] = s
                half[d, :] = p.astype(jnp.bfloat16)

            loop(g, body)
        gather3(g).start()
        put(g, 0)
        for i, a in enumerate(GROUPS[g].members):
            pltpu.make_async_copy(lanes(g, own[g], i), nexts[a], next_sem.at[g]).start()
            pltpu.make_async_copy(lanes(g, st[g], i), news[a], new_sem.at[g]).start()

    def put(g, b):
        for i, a in enumerate(GROUPS[g].members):
            pltpu.make_async_copy(lanes(g, full[g].at[b], i), slab(g, b, halves[a], i), half_sem.at[g]).start()

    def gather3(g):
        return remote(
            full[g].at[0], full[g].at[block(g, 0, 0, 1)], ag_s.at[g, 6], ag_r.at[g, 6], peer_of(g, 3)
        )

    def gather2(g, kt):
        return remote(
            full[g].at[block(g, 0, 0, kt)],
            full[g].at[block(g, 0, 1, kt)],
            ag_s.at[g, 4 + kt],
            ag_r.at[g, 4 + kt],
            peer_of(g, 2),
        )

    def gather1(g, kt, ks):
        i = kt * 2 + ks
        return remote(
            full[g].at[block(g, 0, ks, kt)],
            full[g].at[block(g, 1, ks, kt)],
            ag_s.at[g, i],
            ag_r.at[g, i],
            peer_of(g, 1),
        )

    def spread_own(g):
        gather2(g, 0).start()
        gather1(g, 0, 0).start()

    def got3(g):
        gather3(g).wait_recv()
        gather2(g, 1).start()
        gather1(g, 1, 0).start()
        put(g, block(g, 0, 0, 1))

    def got2(g, kt):
        gather2(g, kt).wait_recv()
        gather1(g, kt, 1).start()
        put(g, block(g, 0, 1, kt))

    def got1(g):
        for kt, ks in ((0, 0), (1, 0), (0, 1), (1, 1)):
            gather1(g, kt, ks).wait_recv()
            put(g, block(g, 1, ks, kt))

    width = vs.shape[1] // replicas

    def vec_out(j):
        to = lax.rem(r + j, replicas)
        return remote(
            vs.at[:, pl.ds(pl.multiple_of(to * width, width), width)],
            vrec.at[j - 1], v_s.at[j - 1], v_r.at[j - 1], to,
        )

    def vec_back(j):
        return remote(vnext, vag.at[j - 1], w_s.at[j - 1], w_r.at[j - 1], lax.rem(r + j, replicas))

    def vec_update():
        pltpu.make_async_copy(vown, vown, vown_sem).wait()
        total = vown[...]
        for j in range(1, replicas):
            vec_out(j).wait_recv()
            total = total + vrec[j - 1]
        v = total * rate
        p, s = rule(param_norm[...], state_norm[...], v[0:1, :])
        next_norm[...] = p
        new_norm[...] = s
        vnext[0:1, :] = p
        p, s = rule(param_bias[...], state_bias[...], v[1:2, :])
        next_bias[...] = p
        new_bias[...] = s
        vnext[1:2, :] = p
        for j in range(1, replicas):
            vec_back(j).start()

    def vec_finish():
        half_norm[r] = vnext[0:1, :].astype(jnp.bfloat16)
        half_bias[r] = vnext[1:2, :].astype(jnp.bfloat16)
        for j in range(1, replicas):
            vec_back(j).wait_recv()
            at = lax.rem(r + replicas - j, replicas)
            half_norm[at] = vag[j - 1, 0:1, :].astype(jnp.bfloat16)
            half_bias[at] = vag[j - 1, 1:2, :].astype(jnp.bfloat16)

    vs[0:1, :] = slope_norm[...]
    vs[1:2, :] = slope_bias[...]
    encode1(UP, 0)
    encode1(QKV, 0)
    pl.semaphore_wait(barrier, replicas + models - 2)
    copy1(UP, 0).start()
    copy1(QKV, 0).start()
    for i in (1, 2, 3):
        encode1(UP, i)
        copy1(UP, i).start()
        encode1(QKV, i)
        copy1(QKV, i).start()
    pltpu.make_async_copy(vs.at[:, pl.ds(pl.multiple_of(r * width, width), width)], vown, vown_sem).start()
    for j in range(1, replicas):
        vec_out(j).start()
    for i in range(4):
        encode1(DOWN, i)
    for i in range(4):
        encode1(MIXED, i)
    for g in groups:
        own_squares(g)
    vec_update()
    take1(QKV, 0)
    take1(QKV, 1)
    for g in (DOWN, MIXED):
        for i in range(4):
            copy1(g, i).start()
    take1(QKV, 2)
    take1(QKV, 3)
    for i in range(4):
        take1(UP, i)
    take2(QKV, 1)
    take2(UP, 1)
    take2(QKV, 0)
    take2(UP, 0)
    take3(QKV)
    take1(DOWN, 0)
    take3(UP)
    update(QKV)
    spread_own(QKV)
    take1(DOWN, 1)
    update(UP)
    spread_own(UP)
    got3(QKV)
    take1(DOWN, 2)
    take1(DOWN, 3)
    take2(DOWN, 1)
    got3(UP)
    got2(QKV, 0)
    for i in range(4):
        take1(MIXED, i)
    take2(DOWN, 0)
    take2(MIXED, 1)
    take2(MIXED, 0)
    got2(QKV, 1)
    take3(DOWN)
    take3(MIXED)
    update(DOWN)
    spread_own(DOWN)
    update(MIXED)
    spread_own(MIXED)
    got2(UP, 0)
    got2(UP, 1)
    got3(DOWN)
    got3(MIXED)
    got2(DOWN, 0)
    got2(MIXED, 0)
    got2(DOWN, 1)
    got2(MIXED, 1)
    vec_finish()
    for g in (QKV, UP, DOWN, MIXED):
        got1(g)

    for g in groups:
        for i in range(4):
            copy1(g, i).wait_send()
        for kt in (0, 1):
            copy2(g, kt).wait_send()
            gather2(g, kt).wait_send()
            for ks in (0, 1):
                gather1(g, kt, ks).wait_send()
        copy3(g).wait_send()
        gather3(g).wait_send()
        for j in range(1, models):
            copyn(g, j).wait_send()
        pltpu.make_async_copy(full[g], full[g], half_sem.at[g]).wait()
        pltpu.make_async_copy(own[g], own[g], next_sem.at[g]).wait()
        pltpu.make_async_copy(st[g], st[g], new_sem.at[g]).wait()
    for j in range(1, replicas):
        vec_out(j).wait_send()
        vec_back(j).wait_send()


def fused(replicas, models, *args):
    slopes, params = args[0:6], args[8:14]
    f32, bf16 = jnp.float32, jnp.bfloat16
    vec = args[6].shape[1]
    width = vec // replicas
    row = lambda a: a.reshape(1, -1)
    args = (*args[0:14], row(args[14]), row(args[15]), *args[16:22], row(args[22]), row(args[23]))
    shapes = []
    for g in GROUPS:
        h, w = params[g.members[0]].shape
        shapes.append((h, w * len(g.members)))
    S = jax.ShapeDtypeStruct
    outs = [S(a.shape[1:], bf16) for a in slopes] + [S((replicas, 1, width), bf16)] * 2
    for _ in range(2):
        outs += [S(a.shape, f32) for a in params] + [S((1, width), f32)] * 2
    ANY, VM = pl.BlockSpec(memory_space=pl.ANY), pl.BlockSpec(memory_space=pltpu.VMEM)
    part = [ANY] * 6 + [VM] * 2
    scratch = []
    for count, dtype in ((8, f32), (4, bf16), (4, bf16), (2, bf16), (2, bf16), (0, bf16), (0, bf16), (0, f32), (0, f32), (8, bf16)):
        scratch += [pltpu.VMEM((count, *s) if count else s, dtype) for s in shapes]
    sq = [(2, len(g.members), s[0], 128) if g.rows else (2, 8, s[1]) for g, s in zip(GROUPS, shapes)]
    scratch += [pltpu.VMEM(s, f32) for s in sq]
    scratch += [pltpu.VMEM((models - 1, *s), f32) for s in sq]
    scratch += [
        pltpu.VMEM((2, vec), f32),
        pltpu.VMEM((2, width), f32),
        pltpu.VMEM((replicas - 1, 2, width), f32),
        pltpu.VMEM((2, width), f32),
        pltpu.VMEM((replicas - 1, 2, width), f32),
    ]
    dma = pltpu.SemaphoreType.DMA
    n = len(GROUPS)
    scratch += [dma((n, 7))] * 4 + [dma((n, models - 1))] * 2 + [dma((replicas - 1,))] * 4
    scratch += [dma((n, 8))] + [dma((n,))] * 5 + [dma(())]
    out = pl.pallas_call(
        functools.partial(kernel, replicas, models, 4.0, shapes),
        out_shape=outs,
        in_specs=part * 3,
        out_specs=part * 3,
        scratch_shapes=scratch,
        compiler_params=pltpu.CompilerParams(
            collective_id=0, has_side_effects=True, vmem_limit_bytes=60 * 1024 * 1024
        ),
    )(*args)
    flat = lambda a: a.reshape(-1)
    return (
        *out[0:6], flat(out[6]), flat(out[7]),
        *out[8:14], flat(out[14]), flat(out[15]),
        *out[16:22], flat(out[22]), flat(out[23]),
    )


def plain(
    slope_up,
    slope_down,
    slope_query,
    slope_key,
    slope_value,
    slope_mixed,
    slope_norm,
    slope_bias,
    param_up,
    param_down,
    param_query,
    param_key,
    param_value,
    param_mixed,
    param_norm,
    param_bias,
    state_up,
    state_down,
    state_query,
    state_key,
    state_value,
    state_mixed,
    state_norm,
    state_bias,
):
    mean_up, mean_down, mean_query, mean_key, mean_value, mean_mixed = (
        lax.psum_scatter(slope_up[0], "replica", scatter_dimension=0, tiled=True),
        lax.psum_scatter(slope_down[0], "replica", scatter_dimension=1, tiled=True),
        lax.psum_scatter(slope_query[0], "replica", scatter_dimension=0, tiled=True),
        lax.psum_scatter(slope_key[0], "replica", scatter_dimension=0, tiled=True),
        lax.psum_scatter(slope_value[0], "replica", scatter_dimension=0, tiled=True),
        lax.psum_scatter(slope_mixed[0], "replica", scatter_dimension=1, tiled=True),
    )
    whole_norm, whole_bias = lax.psum((slope_norm[0], slope_bias[0]), "replica")
    place = lax.axis_index("replica")
    mean_norm = lax.dynamic_slice_in_dim(
        whole_norm, place * param_norm.shape[0], param_norm.shape[0]
    )
    mean_bias = lax.dynamic_slice_in_dim(
        whole_bias, place * param_bias.shape[0], param_bias.shape[0]
    )
    mean_rate = lax.axis_size("replica") ** (-0.5)
    mean_up = mean_up * mean_rate
    mean_down = mean_down * mean_rate
    mean_query = mean_query * mean_rate
    mean_key = mean_key * mean_rate
    mean_value = mean_value * mean_rate
    mean_mixed = mean_mixed * mean_rate
    mean_norm = mean_norm * mean_rate
    mean_bias = mean_bias * mean_rate
    (
        own_up,
        own_down,
        own_query,
        own_key,
        own_value,
        own_mixed,
        slope_up_norm,
        slope_down_norm,
        slope_query_norm,
        slope_key_norm,
        slope_value_norm,
        slope_mixed_norm,
    ) = lax.psum(
        (
            jnp.sum(param_up * param_up, axis=1, keepdims=True),
            jnp.sum(param_down * param_down, axis=0, keepdims=True),
            jnp.sum(param_query * param_query, axis=1, keepdims=True),
            jnp.sum(param_key * param_key, axis=1, keepdims=True),
            jnp.sum(param_value * param_value, axis=1, keepdims=True),
            jnp.sum(param_mixed * param_mixed, axis=0, keepdims=True),
            jnp.sum(mean_up * mean_up, axis=1, keepdims=True),
            jnp.sum(mean_down * mean_down, axis=0, keepdims=True),
            jnp.sum(mean_query * mean_query, axis=1, keepdims=True),
            jnp.sum(mean_key * mean_key, axis=1, keepdims=True),
            jnp.sum(mean_value * mean_value, axis=1, keepdims=True),
            jnp.sum(mean_mixed * mean_mixed, axis=0, keepdims=True),
        ),
        "model",
    )
    mean_up = mean_up * (jnp.sqrt(own_up) * lax.rsqrt(slope_up_norm + 1e-06))
    mean_down = mean_down * (jnp.sqrt(own_down) * lax.rsqrt(slope_down_norm + 1e-06))
    mean_query = mean_query * (jnp.sqrt(own_query) * lax.rsqrt(slope_query_norm + 1e-06))
    mean_key = mean_key * (jnp.sqrt(own_key) * lax.rsqrt(slope_key_norm + 1e-06))
    mean_value = mean_value * (jnp.sqrt(own_value) * lax.rsqrt(slope_value_norm + 1e-06))
    mean_mixed = mean_mixed * (jnp.sqrt(own_mixed) * lax.rsqrt(slope_mixed_norm + 1e-06))
    state_new_up = hold_rate * state_up + (1.0 - hold_rate) * mean_up * mean_up
    next_up = param_up - learn_rate * mean_up * lax.rsqrt(state_new_up + 1e-06)
    state_new_down = hold_rate * state_down + (1.0 - hold_rate) * mean_down * mean_down
    next_down = param_down - learn_rate * mean_down * lax.rsqrt(state_new_down + 1e-06)
    state_new_query = hold_rate * state_query + (1.0 - hold_rate) * mean_query * mean_query
    next_query = param_query - learn_rate * mean_query * lax.rsqrt(state_new_query + 1e-06)
    state_new_key = hold_rate * state_key + (1.0 - hold_rate) * mean_key * mean_key
    next_key = param_key - learn_rate * mean_key * lax.rsqrt(state_new_key + 1e-06)
    state_new_value = hold_rate * state_value + (1.0 - hold_rate) * mean_value * mean_value
    next_value = param_value - learn_rate * mean_value * lax.rsqrt(state_new_value + 1e-06)
    state_new_mixed = hold_rate * state_mixed + (1.0 - hold_rate) * mean_mixed * mean_mixed
    next_mixed = param_mixed - learn_rate * mean_mixed * lax.rsqrt(state_new_mixed + 1e-06)
    state_new_norm = hold_rate * state_norm + (1.0 - hold_rate) * mean_norm * mean_norm
    next_norm = param_norm - learn_rate * mean_norm * lax.rsqrt(state_new_norm + 1e-06)
    state_new_bias = hold_rate * state_bias + (1.0 - hold_rate) * mean_bias * mean_bias
    next_bias = param_bias - learn_rate * mean_bias * lax.rsqrt(state_new_bias + 1e-06)
    half_up, half_down, half_query, half_key, half_value, half_mixed, half_norm, half_bias = (
        lax.all_gather(next_up.astype(jnp.bfloat16), "replica", axis=0, tiled=True),
        lax.all_gather(next_down.astype(jnp.bfloat16), "replica", axis=1, tiled=True),
        lax.all_gather(next_query.astype(jnp.bfloat16), "replica", axis=0, tiled=True),
        lax.all_gather(next_key.astype(jnp.bfloat16), "replica", axis=0, tiled=True),
        lax.all_gather(next_value.astype(jnp.bfloat16), "replica", axis=0, tiled=True),
        lax.all_gather(next_mixed.astype(jnp.bfloat16), "replica", axis=1, tiled=True),
        lax.all_gather(next_norm.astype(jnp.bfloat16), "replica", axis=0, tiled=True),
        lax.all_gather(next_bias.astype(jnp.bfloat16), "replica", axis=0, tiled=True),
    )
    return (
        half_up,
        half_down,
        half_query,
        half_key,
        half_value,
        half_mixed,
        half_norm,
        half_bias,
        next_up,
        next_down,
        next_query,
        next_key,
        next_value,
        next_mixed,
        next_norm,
        next_bias,
        state_new_up,
        state_new_down,
        state_new_query,
        state_new_key,
        state_new_value,
        state_new_mixed,
        state_new_norm,
        state_new_bias,
    )


def solution(mesh):
    replicas, models = mesh.shape["replica"], mesh.shape["model"]

    def local(*args):
        ok = replicas == 2**3 and all(a.shape[k] % 128 == 0 for a in args[8:14] for k in (0, 1))
        if ok and args[14].shape[0] % 128 == 0:
            return fused(replicas, models, *args)
        return plain(*args)

    placed = (
        P("replica", None, "model"),
        P("replica", "model", None),
        P("replica", None, "model"),
        P("replica", None, "model"),
        P("replica", None, "model"),
        P("replica", "model", None),
        P("replica", None),
        P("replica", None),
        P("replica", "model"),
        P("model", "replica"),
        P("replica", "model"),
        P("replica", "model"),
        P("replica", "model"),
        P("model", "replica"),
        P("replica"),
        P("replica"),
        P("replica", "model"),
        P("model", "replica"),
        P("replica", "model"),
        P("replica", "model"),
        P("replica", "model"),
        P("model", "replica"),
        P("replica"),
        P("replica"),
    )
    return jax.shard_map(
        local,
        mesh=mesh,
        in_specs=placed,
        out_specs=(
            P(None, "model"),
            P("model", None),
            P(None, "model"),
            P(None, "model"),
            P(None, "model"),
            P("model", None),
            P(),
            P(),
            P("replica", "model"),
            P("model", "replica"),
            P("replica", "model"),
            P("replica", "model"),
            P("replica", "model"),
            P("model", "replica"),
            P("replica"),
            P("replica"),
            P("replica", "model"),
            P("model", "replica"),
            P("replica", "model"),
            P("replica", "model"),
            P("replica", "model"),
            P("model", "replica"),
            P("replica"),
            P("replica"),
        ),
        check_vma=False,
    )
```

```python
import functools

import jax
import jax.numpy as jnp
from jax import lax
from jax.experimental import pallas as pl
from jax.experimental.pallas import tpu as pltpu
from jax.sharding import PartitionSpec as P

learn_rate = 0.025
hold_rate = 0.7
root = 9
MESH = pl.DeviceIdType.MESH


class Group:
    def __init__(self, members, rows, near_first):
        self.members = members
        self.rows = rows
        self.near_first = near_first


UP, DOWN, MIXED, QKV = range(4)
GROUPS = (
    Group((0,), True, False),
    Group((1,), False, False),
    Group((5,), False, False),
    Group((2, 3, 4), True, True),
)
ORDER = ((1, 1), (0, 1), (1, 0), (0, 0))


def place_of(r, k2, k1, ky):
    bit = lambda v, k: v if k == 0 else 1 - v
    return (bit(r // 4, k2) * 2 + bit((r // 2) % 2, k1)) * 2 + bit(r % 2, ky)


def slab_of(shapes, r, g, b, ref):
    at = place_of(r, b // 4, (b // 2) % 2, b % 2)
    h, w = shapes[g]
    if GROUPS[g].rows:
        return ref.at[pl.ds(pl.multiple_of(at * h, h), h), :]
    return ref.at[:, pl.ds(pl.multiple_of(at * w, w), w)]


def lanes_of(shapes, g, ref, i):
    n = len(GROUPS[g].members)
    w = shapes[g][1] // n
    return ref if n == 1 else ref.at[:, i * w : (i + 1) * w]


def finish(shapes, *refs):
    n = len(GROUPS)
    full, own, st = refs[0:n], refs[n : 2 * n], refs[2 * n : 3 * n]
    vectors = refs[3 * n : 3 * n + 6]
    halves, nexts, news = (refs[3 * n + 6 + 8 * k : 3 * n + 14 + 8 * k] for k in range(3))
    sem, vec_sem = refs[3 * n + 30 :]
    r = lax.axis_index("replica")
    for g, group in enumerate(GROUPS):
        for i, a in enumerate(group.members):
            for b in range(8):
                src = lanes_of(shapes, g, full[g].at[b], i)
                pltpu.make_async_copy(src, slab_of(shapes, r, g, b, halves[a]), sem.at[0, g]).start()
            pltpu.make_async_copy(lanes_of(shapes, g, own[g], i), nexts[a], sem.at[1, g]).start()
            pltpu.make_async_copy(lanes_of(shapes, g, st[g], i), news[a], sem.at[2, g]).start()
    copies = []
    for i, dst in enumerate((*halves[6:], *nexts[6:], *news[6:])):
        copies.append(pltpu.make_async_copy(vectors[i], dst, vec_sem.at[i]))
        copies[-1].start()
    for g in range(n):
        for k, ref in enumerate((full[g], own[g], st[g])):
            pltpu.make_async_copy(ref, ref, sem.at[k, g]).wait()
    for c in copies:
        c.wait()


def kernel(replicas, models, limit, shapes, *refs):
    slopes, slope_norm, slope_bias = refs[0:6], refs[6], refs[7]
    params, param_norm, param_bias = refs[8:14], refs[14], refs[15]
    states, state_norm, state_bias = refs[16:22], refs[22], refs[23]
    groups = range(len(GROUPS))
    n = len(GROUPS)
    full, own, st = refs[24 : 24 + n], refs[24 + n : 24 + 2 * n], refs[24 + 2 * n : 24 + 3 * n]
    half_norm, half_bias, next_norm, next_bias, new_norm, new_bias = refs[24 + 3 * n : 30 + 3 * n]
    scratch = list(refs[30 + 3 * n :])
    take = lambda: [scratch.pop(0) for _ in groups]
    xin, enc1, rec1, enc2, rec2, enc3, rec3, sq, sqr = (take() for _ in range(9))
    vs, vown, vrec, vnext, vag, vh_norm, vh_bias = (scratch.pop(0) for _ in range(7))
    rs_s, rs_r, ag_s, ag_r, n_s, n_r, v_s, v_r, w_s, w_r = (scratch.pop(0) for _ in range(10))
    load_sem, own_sem, st_sem, vown_sem = scratch

    r = lax.axis_index("replica")
    m = lax.axis_index("model")
    place = functools.partial(place_of, r)
    y_peer, near_peer, far_peer = place(0, 0, 1), place(0, 1, 0), place(1, 0, 0)

    scale = 2.0**13 / (limit * replicas)
    rate = replicas ** (-0.5)

    def encode(x):
        t = x * scale
        t2 = t * t
        t4 = t2 * t2
        return (t4 * t4 * t).astype(jnp.bfloat16)

    def decode(c):
        f = c.astype(jnp.float32)
        a = jnp.exp(jnp.log(jnp.abs(f)) * (1.0 / root)) * (1.0 / scale)
        return jnp.where(f < 0, -a, a)

    def block(g, kf, ks, kt):
        return kt * 4 + (kf * 2 + ks if GROUPS[g].near_first else ks * 2 + kf)

    lanes = functools.partial(lanes_of, shapes)
    slab = lambda g, b, ref, i: slab_of(shapes, r, g, b, ref)

    def loop(g, body):
        h, w = shapes[g]
        step = min(h, max(16, 16 * 1024 // w // 16 * 16))
        while h % step:
            step -= 16
        lax.fori_loop(0, h // step, lambda i, c: (body(pl.ds(pl.multiple_of(i * step, step), step)), c)[1], 0)

    def remote(src, dst, s, d, peer, axis="replica"):
        return pltpu.make_async_remote_copy(
            src_ref=src, dst_ref=dst, send_sem=s, recv_sem=d, device_id={axis: peer}, device_id_type=MESH
        )

    barrier = pltpu.get_barrier_semaphore()
    for j in range(1, replicas):
        pl.semaphore_signal(barrier, inc=1, device_id={"replica": lax.rem(r + j, replicas)}, device_id_type=MESH)
    for j in range(1, models):
        pl.semaphore_signal(barrier, inc=1, device_id={"model": lax.rem(m + j, models)}, device_id_type=MESH)

    def load(g, b):
        for i, a in enumerate(GROUPS[g].members):
            pltpu.make_async_copy(
                slab(g, b, slopes[a].at[0], i), lanes(g, xin[g].at[b], i), load_sem.at[g, b]
            ).start()

    def loaded(g, b):
        pltpu.make_async_copy(xin[g].at[b], xin[g].at[b], load_sem.at[g, b]).wait()

    for kt, ks in ORDER:
        load(UP, block(UP, 1, ks, kt))
        load(QKV, block(QKV, 1, ks, kt))
    for kt, ks in ORDER:
        load(QKV, block(QKV, 0, ks, kt))
    for g in (DOWN, MIXED):
        for kt, ks in ORDER:
            load(g, block(g, 1, ks, kt))
    for g in groups:
        for i, a in enumerate(GROUPS[g].members):
            pltpu.make_async_copy(params[a], lanes(g, own[g], i), own_sem.at[g]).start()
            pltpu.make_async_copy(states[a], lanes(g, st[g], i), st_sem.at[g]).start()
    for g in (UP, DOWN, MIXED):
        for kt, ks in ORDER:
            load(g, block(g, 0, ks, kt))

    def peer_of(g, stage):
        if stage == 3:
            return far_peer
        return near_peer if (stage == 1) == GROUPS[g].near_first else y_peer

    def copy1(g, i):
        return remote(enc1[g].at[i], rec1[g].at[i], rs_s.at[g, i], rs_r.at[g, i], peer_of(g, 1))

    def copy2(g, kt):
        return remote(enc2[g].at[kt], rec2[g].at[kt], rs_s.at[g, 4 + kt], rs_r.at[g, 4 + kt], peer_of(g, 2))

    def copy3(g):
        return remote(enc3[g], rec3[g], rs_s.at[g, 6], rs_r.at[g, 6], peer_of(g, 3))

    def encode1(g, i):
        kt, ks = ORDER[i]
        b = block(g, 1, ks, kt)
        loaded(g, b)
        src, dst = xin[g].at[b], enc1[g].at[i]

        def body(d):
            dst[d, :] = encode(src[d, :])

        loop(g, body)

    def add(g, b, rec):
        acc = xin[g].at[b]

        def body(d):
            acc[d, :] = acc[d, :] + decode(rec[d, :])

        loop(g, body)

    def add_encode(g, b, rec, dst):
        acc = xin[g].at[b]

        def body(d):
            dst[d, :] = encode(acc[d, :] + decode(rec[d, :]))

        loop(g, body)

    def take1(g, i):
        kt, ks = ORDER[i]
        b = block(g, 0, ks, kt)
        loaded(g, b)
        copy1(g, i).wait_recv()
        if ks:
            add_encode(g, b, rec1[g].at[i], enc2[g].at[kt])
            copy2(g, kt).start()
        else:
            add(g, b, rec1[g].at[i])

    def take2(g, kt):
        b = block(g, 0, 0, kt)
        copy2(g, kt).wait_recv()
        if kt:
            add_encode(g, b, rec2[g].at[kt], enc3[g])
            copy3(g).start()
        else:
            add(g, b, rec2[g].at[kt])

    def fold(x):
        w = x.shape[1]
        total = x[:, 0:128]
        for k in range(128, w, 128):
            total = total + x[:, k : k + 128]
        return total

    def squares(g, which, read):
        h, w = shapes[g]
        if GROUPS[g].rows:
            n = len(GROUPS[g].members)

            def body(d):
                v = read(d)
                v = v * v
                for i in range(n):
                    sq[g][which, i, d, :] = fold(v[:, i * (w // n) : (i + 1) * (w // n)])

            loop(g, body)
        else:
            sq[g][which] = jnp.zeros((8, w), jnp.float32)

            def body(d):
                v = read(d)
                sq[g][which] += jnp.sum((v * v).reshape(-1, 8, w), axis=0)

            loop(g, body)

    def copyn(g, j):
        return remote(
            sq[g], sqr[g].at[j - 1], n_s.at[g, j - 1], n_r.at[g, j - 1], lax.rem(m + j, models), "model"
        )

    def own_squares(g):
        pltpu.make_async_copy(own[g], own[g], own_sem.at[g]).wait()
        squares(g, 0, lambda d: own[g][d, :])

    def take3(g):
        copy3(g).wait_recv()
        acc, rec = xin[g].at[0], rec3[g]

        def read(d):
            v = (acc[d, :] + decode(rec[d, :])) * rate
            acc[d, :] = v
            return v

        squares(g, 1, read)
        for j in range(1, models):
            copyn(g, j).start()

    def rule(p, s, v):
        s = hold_rate * s + (1.0 - hold_rate) * v * v
        return p - learn_rate * v * lax.rsqrt(s + 1e-06), s

    def update(g):
        h, w = shapes[g]
        for j in range(1, models):
            copyn(g, j).wait_recv()
        pltpu.make_async_copy(st[g], st[g], st_sem.at[g]).wait()
        acc, half = xin[g].at[0], full[g].at[0]

        def ratio(index, axis):
            p, s = sq[g][(0, *index)], sq[g][(1, *index)]
            for j in range(models - 1):
                p = p + sqr[g][(j, 0, *index)]
                s = s + sqr[g][(j, 1, *index)]
            p = jnp.sum(p, axis=axis, keepdims=True)
            s = jnp.sum(s, axis=axis, keepdims=True)
            return jnp.sqrt(p) * lax.rsqrt(s + 1e-06)

        if GROUPS[g].rows:
            n = len(GROUPS[g].members)

            def body(d):
                for i in range(n):
                    cols = slice(i * (w // n), (i + 1) * (w // n))
                    v = acc[d, cols] * ratio((i, d), 1)
                    p, s = rule(own[g][d, cols], st[g][d, cols], v)
                    own[g][d, cols] = p
                    st[g][d, cols] = s
                    half[d, cols] = p.astype(jnp.bfloat16)

            loop(g, body)
        else:
            t = ratio((), 0)

            def body(d):
                p, s = rule(own[g][d, :], st[g][d, :], acc[d, :] * t)
                own[g][d, :] = p
                st[g][d, :] = s
                half[d, :] = p.astype(jnp.bfloat16)

            loop(g, body)
        gather3(g).start()

    def gather3(g):
        return remote(
            full[g].at[0], full[g].at[block(g, 0, 0, 1)], ag_s.at[g, 6], ag_r.at[g, 6], peer_of(g, 3)
        )

    def gather2(g, kt):
        return remote(
            full[g].at[block(g, 0, 0, kt)],
            full[g].at[block(g, 0, 1, kt)],
            ag_s.at[g, 4 + kt],
            ag_r.at[g, 4 + kt],
            peer_of(g, 2),
        )

    def gather1(g, kt, ks):
        i = kt * 2 + ks
        return remote(
            full[g].at[block(g, 0, ks, kt)],
            full[g].at[block(g, 1, ks, kt)],
            ag_s.at[g, i],
            ag_r.at[g, i],
            peer_of(g, 1),
        )

    def spread_own(g):
        gather2(g, 0).start()
        gather1(g, 0, 0).start()

    def got3(g):
        gather3(g).wait_recv()
        gather2(g, 1).start()
        gather1(g, 1, 0).start()

    def got2(g, kt):
        gather2(g, kt).wait_recv()
        gather1(g, kt, 1).start()

    def got1(g):
        for kt, ks in ((0, 0), (1, 0), (0, 1), (1, 1)):
            gather1(g, kt, ks).wait_recv()

    width = vs.shape[1] // replicas

    def vec_out(j):
        to = lax.rem(r + j, replicas)
        return remote(
            vs.at[:, pl.ds(pl.multiple_of(to * width, width), width)],
            vrec.at[j - 1], v_s.at[j - 1], v_r.at[j - 1], to,
        )

    def vec_back(j):
        return remote(vnext, vag.at[j - 1], w_s.at[j - 1], w_r.at[j - 1], lax.rem(r + j, replicas))

    def vec_update():
        pltpu.make_async_copy(vown, vown, vown_sem).wait()
        total = vown[...]
        for j in range(1, replicas):
            vec_out(j).wait_recv()
            total = total + vrec[j - 1]
        v = total * rate
        p, s = rule(param_norm[...], state_norm[...], v[0:1, :])
        next_norm[...] = p
        new_norm[...] = s
        vnext[0:1, :] = p
        p, s = rule(param_bias[...], state_bias[...], v[1:2, :])
        next_bias[...] = p
        new_bias[...] = s
        vnext[1:2, :] = p
        for j in range(1, replicas):
            vec_back(j).start()

    def vec_finish():
        vh_norm[pl.ds(r, 1), :] = vnext[0:1, :]
        vh_bias[pl.ds(r, 1), :] = vnext[1:2, :]
        for j in range(1, replicas):
            vec_back(j).wait_recv()
            at = lax.rem(r + replicas - j, replicas)
            vh_norm[pl.ds(at, 1), :] = vag[j - 1, 0:1, :]
            vh_bias[pl.ds(at, 1), :] = vag[j - 1, 1:2, :]
        half_norm[...] = vh_norm[...].astype(jnp.bfloat16)
        half_bias[...] = vh_bias[...].astype(jnp.bfloat16)

    vs[0:1, :] = slope_norm[...]
    vs[1:2, :] = slope_bias[...]
    encode1(UP, 0)
    encode1(QKV, 0)
    pl.semaphore_wait(barrier, replicas + models - 2)
    copy1(UP, 0).start()
    copy1(QKV, 0).start()
    for i in (1, 2, 3):
        encode1(UP, i)
        copy1(UP, i).start()
        encode1(QKV, i)
        copy1(QKV, i).start()
    pltpu.make_async_copy(vs.at[:, pl.ds(pl.multiple_of(r * width, width), width)], vown, vown_sem).start()
    for j in range(1, replicas):
        vec_out(j).start()
    for i in range(4):
        encode1(DOWN, i)
    for i in range(4):
        encode1(MIXED, i)
    for g in groups:
        own_squares(g)
    vec_update()
    take1(QKV, 0)
    take1(QKV, 1)
    for g in (DOWN, MIXED):
        for i in range(4):
            copy1(g, i).start()
    take1(QKV, 2)
    take1(QKV, 3)
    for i in range(4):
        take1(UP, i)
    take2(QKV, 1)
    take2(UP, 1)
    take2(QKV, 0)
    take2(UP, 0)
    take3(QKV)
    take1(DOWN, 0)
    take3(UP)
    update(QKV)
    spread_own(QKV)
    take1(DOWN, 1)
    update(UP)
    spread_own(UP)
    got3(QKV)
    take1(DOWN, 2)
    take1(DOWN, 3)
    take2(DOWN, 1)
    got3(UP)
    got2(QKV, 0)
    for i in range(4):
        take1(MIXED, i)
    take2(DOWN, 0)
    take2(MIXED, 1)
    take2(MIXED, 0)
    got2(QKV, 1)
    take3(DOWN)
    take3(MIXED)
    update(DOWN)
    spread_own(DOWN)
    update(MIXED)
    spread_own(MIXED)
    got2(UP, 0)
    got2(UP, 1)
    got3(DOWN)
    got3(MIXED)
    got2(DOWN, 0)
    got2(MIXED, 0)
    got2(DOWN, 1)
    got2(MIXED, 1)
    vec_finish()
    for g in (QKV, UP, DOWN, MIXED):
        got1(g)

    for g in groups:
        for i in range(4):
            copy1(g, i).wait_send()
        for kt in (0, 1):
            copy2(g, kt).wait_send()
            gather2(g, kt).wait_send()
            for ks in (0, 1):
                gather1(g, kt, ks).wait_send()
        copy3(g).wait_send()
        gather3(g).wait_send()
        for j in range(1, models):
            copyn(g, j).wait_send()
    for j in range(1, replicas):
        vec_out(j).wait_send()
        vec_back(j).wait_send()


def fused(replicas, models, *args):
    slopes, params = args[0:6], args[8:14]
    f32, bf16 = jnp.float32, jnp.bfloat16
    vec = args[6].shape[1]
    width = vec // replicas
    row = lambda a: a.reshape(1, -1)
    args = (*args[0:14], row(args[14]), row(args[15]), *args[16:22], row(args[22]), row(args[23]))
    shapes = []
    for g in GROUPS:
        h, w = params[g.members[0]].shape
        shapes.append((h, w * len(g.members)))
    S = jax.ShapeDtypeStruct
    n = len(GROUPS)
    held = [((replicas, *s), bf16) for s in shapes] + [(s, f32) for s in shapes] * 2
    held += [((replicas, width), bf16)] * 2 + [((1, width), f32)] * 4
    ANY, VM = pl.BlockSpec(memory_space=pl.ANY), pl.BlockSpec(memory_space=pltpu.VMEM)
    part = [ANY] * 6 + [VM] * 2
    scratch = []
    for count, dtype in ((8, f32), (4, bf16), (4, bf16), (2, bf16), (2, bf16), (0, bf16), (0, bf16)):
        scratch += [pltpu.VMEM((count, *s) if count else s, dtype) for s in shapes]
    sq = [(2, len(g.members), s[0], 128) if g.rows else (2, 8, s[1]) for g, s in zip(GROUPS, shapes)]
    scratch += [pltpu.VMEM(s, f32) for s in sq]
    scratch += [pltpu.VMEM((models - 1, *s), f32) for s in sq]
    scratch += [
        pltpu.VMEM((2, vec), f32),
        pltpu.VMEM((2, width), f32),
        pltpu.VMEM((replicas - 1, 2, width), f32),
        pltpu.VMEM((2, width), f32),
        pltpu.VMEM((replicas - 1, 2, width), f32),
        pltpu.VMEM((replicas, width), f32),
        pltpu.VMEM((replicas, width), f32),
    ]
    dma = pltpu.SemaphoreType.DMA
    scratch += [dma((n, 7))] * 4 + [dma((n, models - 1))] * 2 + [dma((replicas - 1,))] * 4
    scratch += [dma((n, 8))] + [dma((n,))] * 2 + [dma(())]
    out = pl.pallas_call(
        functools.partial(kernel, replicas, models, 4.0, shapes),
        out_shape=[pltpu.VMEM(*h) for h in held],
        in_specs=part * 3,
        out_specs=[VM] * len(held),
        scratch_shapes=scratch,
        compiler_params=pltpu.CompilerParams(
            collective_id=0, has_side_effects=True, vmem_limit_bytes=54 * 1024 * 1024
        ),
    )(*args)
    outs = [S(a.shape[1:], bf16) for a in slopes] + [S((replicas, width), bf16)] * 2
    for _ in range(2):
        outs += [S(a.shape, f32) for a in params] + [S((1, width), f32)] * 2
    out = pl.pallas_call(
        functools.partial(finish, shapes),
        out_shape=outs,
        in_specs=[VM] * len(held),
        out_specs=[ANY] * len(outs),
        scratch_shapes=[dma((3, n)), dma((6,))],
        compiler_params=pltpu.CompilerParams(vmem_limit_bytes=1024 * 1024),
    )(*out)
    flat = lambda a: a.reshape(-1)
    return (
        *out[0:6], flat(out[6]), flat(out[7]),
        *out[8:14], flat(out[14]), flat(out[15]),
        *out[16:22], flat(out[22]), flat(out[23]),
    )


def plain(
    slope_up,
    slope_down,
    slope_query,
    slope_key,
    slope_value,
    slope_mixed,
    slope_norm,
    slope_bias,
    param_up,
    param_down,
    param_query,
    param_key,
    param_value,
    param_mixed,
    param_norm,
    param_bias,
    state_up,
    state_down,
    state_query,
    state_key,
    state_value,
    state_mixed,
    state_norm,
    state_bias,
):
    mean_up, mean_down, mean_query, mean_key, mean_value, mean_mixed = (
        lax.psum_scatter(slope_up[0], "replica", scatter_dimension=0, tiled=True),
        lax.psum_scatter(slope_down[0], "replica", scatter_dimension=1, tiled=True),
        lax.psum_scatter(slope_query[0], "replica", scatter_dimension=0, tiled=True),
        lax.psum_scatter(slope_key[0], "replica", scatter_dimension=0, tiled=True),
        lax.psum_scatter(slope_value[0], "replica", scatter_dimension=0, tiled=True),
        lax.psum_scatter(slope_mixed[0], "replica", scatter_dimension=1, tiled=True),
    )
    whole_norm, whole_bias = lax.psum((slope_norm[0], slope_bias[0]), "replica")
    place = lax.axis_index("replica")
    mean_norm = lax.dynamic_slice_in_dim(
        whole_norm, place * param_norm.shape[0], param_norm.shape[0]
    )
    mean_bias = lax.dynamic_slice_in_dim(
        whole_bias, place * param_bias.shape[0], param_bias.shape[0]
    )
    mean_rate = lax.axis_size("replica") ** (-0.5)
    mean_up = mean_up * mean_rate
    mean_down = mean_down * mean_rate
    mean_query = mean_query * mean_rate
    mean_key = mean_key * mean_rate
    mean_value = mean_value * mean_rate
    mean_mixed = mean_mixed * mean_rate
    mean_norm = mean_norm * mean_rate
    mean_bias = mean_bias * mean_rate
    (
        own_up,
        own_down,
        own_query,
        own_key,
        own_value,
        own_mixed,
        slope_up_norm,
        slope_down_norm,
        slope_query_norm,
        slope_key_norm,
        slope_value_norm,
        slope_mixed_norm,
    ) = lax.psum(
        (
            jnp.sum(param_up * param_up, axis=1, keepdims=True),
            jnp.sum(param_down * param_down, axis=0, keepdims=True),
            jnp.sum(param_query * param_query, axis=1, keepdims=True),
            jnp.sum(param_key * param_key, axis=1, keepdims=True),
            jnp.sum(param_value * param_value, axis=1, keepdims=True),
            jnp.sum(param_mixed * param_mixed, axis=0, keepdims=True),
            jnp.sum(mean_up * mean_up, axis=1, keepdims=True),
            jnp.sum(mean_down * mean_down, axis=0, keepdims=True),
            jnp.sum(mean_query * mean_query, axis=1, keepdims=True),
            jnp.sum(mean_key * mean_key, axis=1, keepdims=True),
            jnp.sum(mean_value * mean_value, axis=1, keepdims=True),
            jnp.sum(mean_mixed * mean_mixed, axis=0, keepdims=True),
        ),
        "model",
    )
    mean_up = mean_up * (jnp.sqrt(own_up) * lax.rsqrt(slope_up_norm + 1e-06))
    mean_down = mean_down * (jnp.sqrt(own_down) * lax.rsqrt(slope_down_norm + 1e-06))
    mean_query = mean_query * (jnp.sqrt(own_query) * lax.rsqrt(slope_query_norm + 1e-06))
    mean_key = mean_key * (jnp.sqrt(own_key) * lax.rsqrt(slope_key_norm + 1e-06))
    mean_value = mean_value * (jnp.sqrt(own_value) * lax.rsqrt(slope_value_norm + 1e-06))
    mean_mixed = mean_mixed * (jnp.sqrt(own_mixed) * lax.rsqrt(slope_mixed_norm + 1e-06))
    state_new_up = hold_rate * state_up + (1.0 - hold_rate) * mean_up * mean_up
    next_up = param_up - learn_rate * mean_up * lax.rsqrt(state_new_up + 1e-06)
    state_new_down = hold_rate * state_down + (1.0 - hold_rate) * mean_down * mean_down
    next_down = param_down - learn_rate * mean_down * lax.rsqrt(state_new_down + 1e-06)
    state_new_query = hold_rate * state_query + (1.0 - hold_rate) * mean_query * mean_query
    next_query = param_query - learn_rate * mean_query * lax.rsqrt(state_new_query + 1e-06)
    state_new_key = hold_rate * state_key + (1.0 - hold_rate) * mean_key * mean_key
    next_key = param_key - learn_rate * mean_key * lax.rsqrt(state_new_key + 1e-06)
    state_new_value = hold_rate * state_value + (1.0 - hold_rate) * mean_value * mean_value
    next_value = param_value - learn_rate * mean_value * lax.rsqrt(state_new_value + 1e-06)
    state_new_mixed = hold_rate * state_mixed + (1.0 - hold_rate) * mean_mixed * mean_mixed
    next_mixed = param_mixed - learn_rate * mean_mixed * lax.rsqrt(state_new_mixed + 1e-06)
    state_new_norm = hold_rate * state_norm + (1.0 - hold_rate) * mean_norm * mean_norm
    next_norm = param_norm - learn_rate * mean_norm * lax.rsqrt(state_new_norm + 1e-06)
    state_new_bias = hold_rate * state_bias + (1.0 - hold_rate) * mean_bias * mean_bias
    next_bias = param_bias - learn_rate * mean_bias * lax.rsqrt(state_new_bias + 1e-06)
    half_up, half_down, half_query, half_key, half_value, half_mixed, half_norm, half_bias = (
        lax.all_gather(next_up.astype(jnp.bfloat16), "replica", axis=0, tiled=True),
        lax.all_gather(next_down.astype(jnp.bfloat16), "replica", axis=1, tiled=True),
        lax.all_gather(next_query.astype(jnp.bfloat16), "replica", axis=0, tiled=True),
        lax.all_gather(next_key.astype(jnp.bfloat16), "replica", axis=0, tiled=True),
        lax.all_gather(next_value.astype(jnp.bfloat16), "replica", axis=0, tiled=True),
        lax.all_gather(next_mixed.astype(jnp.bfloat16), "replica", axis=1, tiled=True),
        lax.all_gather(next_norm.astype(jnp.bfloat16), "replica", axis=0, tiled=True),
        lax.all_gather(next_bias.astype(jnp.bfloat16), "replica", axis=0, tiled=True),
    )
    return (
        half_up,
        half_down,
        half_query,
        half_key,
        half_value,
        half_mixed,
        half_norm,
        half_bias,
        next_up,
        next_down,
        next_query,
        next_key,
        next_value,
        next_mixed,
        next_norm,
        next_bias,
        state_new_up,
        state_new_down,
        state_new_query,
        state_new_key,
        state_new_value,
        state_new_mixed,
        state_new_norm,
        state_new_bias,
    )


def solution(mesh):
    replicas, models = mesh.shape["replica"], mesh.shape["model"]

    def local(*args):
        ok = replicas == 2**3 and all(a.shape[k] % 128 == 0 for a in args[8:14] for k in (0, 1))
        if ok and args[14].shape[0] % 128 == 0:
            return fused(replicas, models, *args)
        return plain(*args)

    placed = (
        P("replica", None, "model"),
        P("replica", "model", None),
        P("replica", None, "model"),
        P("replica", None, "model"),
        P("replica", None, "model"),
        P("replica", "model", None),
        P("replica", None),
        P("replica", None),
        P("replica", "model"),
        P("model", "replica"),
        P("replica", "model"),
        P("replica", "model"),
        P("replica", "model"),
        P("model", "replica"),
        P("replica"),
        P("replica"),
        P("replica", "model"),
        P("model", "replica"),
        P("replica", "model"),
        P("replica", "model"),
        P("replica", "model"),
        P("model", "replica"),
        P("replica"),
        P("replica"),
    )
    return jax.shard_map(
        local,
        mesh=mesh,
        in_specs=placed,
        out_specs=(
            P(None, "model"),
            P("model", None),
            P(None, "model"),
            P(None, "model"),
            P(None, "model"),
            P("model", None),
            P(),
            P(),
            P("replica", "model"),
            P("model", "replica"),
            P("replica", "model"),
            P("replica", "model"),
            P("replica", "model"),
            P("model", "replica"),
            P("replica"),
            P("replica"),
            P("replica", "model"),
            P("model", "replica"),
            P("replica", "model"),
            P("replica", "model"),
            P("replica", "model"),
            P("model", "replica"),
            P("replica"),
            P("replica"),
        ),
        check_vma=False,
    )
```
